32 devices in a mesh: ep: 32 (over z, y, x, core).
Axes of the slice: x: 2, y: 2, z: 4, core: 2. Of those that a mesh axis runs over, the one named last changes fastest.
Arguments:
- hidden: bfloat16 [32768, 1024], P('ep')
- grad_out: bfloat16 [32768, 1024], P('ep')
- w_router: bfloat16 [1024, 32], replicated
- b_router: float32 [32], replicated
- expert_ids: int32 [32768, 8], P('ep')
- slot_ids: int32 [32768, 8], P('ep')
- w_gate_up: bfloat16 [32, 1024, 1024], P('ep')
- b_gate_up: float32 [32, 1024], P('ep')
- w_down: bfloat16 [32, 512, 1024], P('ep')
- b_down: float32 [32, 1024], P('ep')
Outputs:
- output 1: bfloat16 [32768, 1024], P('ep')
- output 2: bfloat16 [32768, 1024], P('ep')
- output 3: float32 [1024, 32], replicated
- output 4: float32 [32], replicated
- output 5: float32 [32, 1024, 1024], P('ep')
- output 6: float32 [32, 1024], P('ep')
- output 7: float32 [32, 512, 1024], P('ep')
- output 8: float32 [32, 1024], P('ep')
All inputs are finite; a program needn't handle non-finite values.
Results may differ from the reference program's by a relative error of at most 0.00975927.
Values are sent between devices in bfloat16 or wider.
A program may use at most 1 GiB of HBM per device.

```python
import jax
import jax.numpy as jnp
from jax import lax

D_MODEL = 1024
FF_EXPERT = 512
EXPERTS = 32
TOP_K = 8
TOKENS_DEV = 1024
EP_DEVICES = 32

TOKENS = EP_DEVICES * TOKENS_DEV
CAPACITY = (3 * TOKENS_DEV * TOP_K + 2 * EXPERTS - 1) // (2 * EXPERTS)
ROWS_EXPERT = EP_DEVICES * CAPACITY
SWIGLU_LIMIT = 7.0
SWIGLU_ALPHA = 1.702


def draw_routing(key):
    key_bias, key_dev = jax.random.split(key)
    expert_bias = jax.random.randint(key_bias, (EXPERTS,), 0, 512)
    expert_range = jnp.arange(EXPERTS, dtype=jnp.int32)
    copies = TOKENS_DEV * TOP_K

    def one_device(dev_key):
        key_noise, key_hot, key_pick, key_prio = jax.random.split(dev_key, 4)
        noise_int = jax.random.randint(key_noise, (TOKENS_DEV, EXPERTS), 0, 1024)
        hot_expert = jax.random.randint(key_hot, (), 0, EXPERTS)
        forced = jax.random.permutation(key_pick, TOKENS_DEV) < 2 * CAPACITY
        hot_bonus = jnp.where(forced[:, None] & (expert_range[None, :] == hot_expert), 4096, 0)
        scores = (noise_int + expert_bias[None, :] + hot_bonus) * EXPERTS + expert_range[None, :]
        choice = lax.top_k(scores, TOP_K)[1].astype(jnp.int32)
        flat_ids = choice.reshape(-1)
        priority = jax.random.permutation(key_prio, copies)
        sort_order = jnp.argsort(flat_ids * copies + priority)
        counts = jnp.bincount(flat_ids, length=EXPERTS)
        starts = jnp.cumsum(counts) - counts
        rank_sorted = (jnp.arange(copies, dtype=jnp.int32) - starts[flat_ids[sort_order]]).astype(jnp.int32)
        slot_rank = jnp.zeros((copies,), jnp.int32).at[sort_order].set(rank_sorted)
        slot_ids = jnp.where(slot_rank < CAPACITY, slot_rank, -1).reshape(TOKENS_DEV, TOP_K)
        return choice, slot_ids

    choice, slot_ids = jax.vmap(one_device)(jax.random.split(key_dev, EP_DEVICES))
    return choice.reshape(TOKENS, TOP_K), slot_ids.reshape(TOKENS, TOP_K).astype(jnp.int32)


def setup_inputs(seed: int = 0) -> dict:
    key_list = jax.random.split(jax.random.key(seed), 9)
    hidden = jax.random.normal(key_list[0], (TOKENS, D_MODEL), jnp.float32).astype(jnp.bfloat16)
    grad_out = jax.random.normal(key_list[1], (TOKENS, D_MODEL), jnp.float32).astype(jnp.bfloat16)
    w_router = (2.0 * D_MODEL ** -0.5 * jax.random.normal(key_list[2], (D_MODEL, EXPERTS), jnp.float32)).astype(jnp.bfloat16)
    b_router = jax.random.normal(key_list[3], (EXPERTS,), jnp.float32)
    expert_ids, slot_ids = draw_routing(key_list[4])
    w_gate_up = (3.0 * D_MODEL ** -0.5 * jax.random.normal(key_list[5], (EXPERTS, D_MODEL, 2 * FF_EXPERT), jnp.float32)).astype(jnp.bfloat16)
    b_gate_up = jax.random.normal(key_list[6], (EXPERTS, 2 * FF_EXPERT), jnp.float32)
    w_down = (0.15 * FF_EXPERT ** -0.5 * jax.random.normal(key_list[7], (EXPERTS, FF_EXPERT, D_MODEL), jnp.float32)).astype(jnp.bfloat16)
    b_down = 0.5 * jax.random.normal(key_list[8], (EXPERTS, D_MODEL), jnp.float32)
    return {'hidden': hidden, 'grad_out': grad_out, 'w_router': w_router, 'b_router': b_router, 'expert_ids': expert_ids, 'slot_ids': slot_ids, 'w_gate_up': w_gate_up, 'b_gate_up': b_gate_up, 'w_down': w_down, 'b_down': b_down}


def swiglu(pre_act):
    col_pairs = pre_act.reshape(pre_act.shape[:-1] + (pre_act.shape[-1] // 2, 2))
    gate_in = jnp.minimum(col_pairs[..., 0], SWIGLU_LIMIT)
    up_in = jnp.clip(col_pairs[..., 1], -SWIGLU_LIMIT, SWIGLU_LIMIT)
    return gate_in * jax.nn.sigmoid(SWIGLU_ALPHA * gate_in) * (up_in + 1.0)


def reference(hidden, grad_out, w_router, b_router, expert_ids, slot_ids, w_gate_up, b_gate_up, w_down, b_down):
    buf_total = EXPERTS * ROWS_EXPERT
    copy_count = TOKENS * TOP_K
    src_dev = (jnp.arange(TOKENS, dtype=jnp.int32) // TOKENS_DEV)[:, None]
    dest_row = jnp.where(slot_ids >= 0, expert_ids * ROWS_EXPERT + src_dev * CAPACITY + slot_ids, buf_total)
    src_copy = jnp.full((buf_total + 1,), copy_count, jnp.int32).at[dest_row.reshape(-1)].set(jnp.arange(copy_count, dtype=jnp.int32))[:buf_total].reshape(EXPERTS, ROWS_EXPERT)
    logits = jnp.dot(hidden, w_router, preferred_element_type=jnp.float32) + b_router
    gate_w = jax.nn.softmax(jnp.take_along_axis(logits, expert_ids, axis=1), axis=-1)
    flat_gate = gate_w.reshape(-1)

    def expert_forward(expert_args):
        w_gu, b_gu, w_dn, b_dn, src_rows = expert_args
        x_rows = jnp.take(hidden, src_rows // TOP_K, axis=0, mode='fill', fill_value=0)
        pre_act = jnp.dot(x_rows, w_gu, preferred_element_type=jnp.float32) + b_gu
        act_bf = swiglu(pre_act).astype(jnp.bfloat16)
        return (jnp.dot(act_bf, w_dn, preferred_element_type=jnp.float32) + b_dn).astype(jnp.bfloat16)

    y_flat = lax.map(expert_forward, (w_gate_up, b_gate_up, w_down, b_down, src_copy)).reshape(buf_total, D_MODEL)

    def token_forward(block_args):
        gate_blk, dest_blk, grad_blk = block_args
        y_blk = jnp.take(y_flat, dest_blk, axis=0, mode='fill', fill_value=0).astype(jnp.float32)
        out_blk = jnp.sum(gate_blk[:, :, None] * y_blk, axis=1).astype(jnp.bfloat16)
        return out_blk, jnp.einsum('td,tkd->tk', grad_blk.astype(jnp.float32), y_blk)

    dev_shape = (EP_DEVICES, TOKENS_DEV)
    block_out, gate_grad = lax.map(token_forward, (gate_w.reshape(dev_shape + (TOP_K,)), dest_row.reshape(dev_shape + (TOP_K,)), grad_out.reshape(dev_shape + (D_MODEL,))))
    block_out = block_out.reshape(TOKENS, D_MODEL)
    gate_grad = gate_grad.reshape(TOKENS, TOP_K)
    sel_grad = gate_w * (gate_grad - jnp.sum(gate_w * gate_grad, axis=1, keepdims=True))
    logit_grad = jnp.zeros((TOKENS, EXPERTS), jnp.float32).at[jnp.arange(TOKENS)[:, None], expert_ids].add(sel_grad).astype(jnp.bfloat16)

    def expert_backward(expert_args):
        w_gu, b_gu, w_dn, src_rows = expert_args
        tok_rows = src_rows // TOP_K
        x_rows = jnp.take(hidden, tok_rows, axis=0, mode='fill', fill_value=0)
        pre_act = jnp.dot(x_rows, w_gu, preferred_element_type=jnp.float32) + b_gu
        act_val, act_vjp = jax.vjp(swiglu, pre_act)
        act_bf = act_val.astype(jnp.bfloat16)
        row_gate = jnp.take(flat_gate, src_rows, axis=0, mode='fill', fill_value=0)
        row_grad = jnp.take(grad_out, tok_rows, axis=0, mode='fill', fill_value=0).astype(jnp.float32)
        q_rows = (row_gate[:, None] * row_grad).astype(jnp.bfloat16)
        grad_b_dn = jnp.sum(q_rows.astype(jnp.float32), axis=0)
        grad_w_dn = jnp.dot(act_bf.T, q_rows, preferred_element_type=jnp.float32)
        act_grad = jnp.dot(q_rows, w_dn.T, preferred_element_type=jnp.float32)
        pre_grad = act_vjp(act_grad)[0].astype(jnp.bfloat16)
        grad_b_gu = jnp.sum(pre_grad.astype(jnp.float32), axis=0)
        grad_w_gu = jnp.dot(x_rows.T, pre_grad, preferred_element_type=jnp.float32)
        p_rows = jnp.dot(pre_grad, w_gu.T, preferred_element_type=jnp.float32).astype(jnp.bfloat16)
        return grad_w_gu, grad_b_gu, grad_w_dn, grad_b_dn, p_rows

    grad_w_gate_up, grad_b_gate_up, grad_w_down, grad_b_down, p_rows = lax.map(expert_backward, (w_gate_up, b_gate_up, w_down, src_copy))
    p_flat = p_rows.reshape(buf_total, D_MODEL)

    def token_backward(block_args):
        dest_blk, logit_blk = block_args
        p_blk = jnp.take(p_flat, dest_blk, axis=0, mode='fill', fill_value=0).astype(jnp.float32)
        router_dx = jnp.dot(logit_blk, w_router.T, preferred_element_type=jnp.float32)
        return (jnp.sum(p_blk, axis=1) + router_dx).astype(jnp.bfloat16)

    grad_hidden = lax.map(token_backward, (dest_row.reshape(dev_shape + (TOP_K,)), logit_grad.reshape(dev_shape + (EXPERTS,)))).reshape(TOKENS, D_MODEL)
    grad_w_router = jnp.dot(hidden.T, logit_grad, preferred_element_type=jnp.float32)
    grad_b_router = jnp.sum(logit_grad.astype(jnp.float32), axis=0)
    return (block_out, grad_hidden, grad_w_router, grad_b_router, grad_w_gate_up, grad_b_gate_up, grad_w_down, grad_b_down)
```

```python
import functools

import jax
import jax.numpy as jnp
from jax import lax
from jax.experimental import pallas as pl
from jax.experimental.pallas import tpu as pltpu
from jax.sharding import PartitionSpec as P

LIMIT = 7.0
ALPHA = 1.702
F32 = jnp.float32
BF16 = jnp.bfloat16
PLANE = 8
DEPTH = 4
VMEM_LIMIT = 62 * 1024 * 1024


def dot(a, b, dims=((1,), (0,))):
    return lax.dot_general(a, b, (dims, ((), ())), preferred_element_type=F32)


def place(me):
    c = me % PLANE
    core, xb, yb = c % 2, (c // 2) % 2, c // 4
    return c, me + 1 - 2 * core, me + 2 - 4 * xb, me + 4 - 8 * yb


def gather_kernel(world, x_ref, dy_ref, meta_ref, bias_ref, xall, dyall, metaall, biasall,
                  send, recv, msend, mrecv, bsend, brecv, local):
    me = lax.axis_index('ep')
    c, partner, xn, yn = place(me)
    base = me - c
    plane_peers = [base + (c + k) % PLANE for k in range(1, PLANE)]
    col_peers = [(me + PLANE * k) % world for k in range(1, DEPTH)]
    cx, cy = xn - base, yn - base
    cd = cx + cy - c
    half = x_ref.shape[0] // 2

    barrier = pltpu.get_barrier_semaphore()
    for peer in plane_peers + col_peers:
        pl.semaphore_signal(barrier, inc=1, device_id=(peer,), device_id_type=pl.DeviceIdType.MESH)
    pl.semaphore_wait(barrier, len(plane_peers) + len(col_peers))

    refs = ((x_ref, xall), (dy_ref, dyall))

    def copy(a, kind, src, blk, h, dev):
        rows = pl.ds(h * half, half)
        source = refs[a][0].at[rows] if src is None else refs[a][1].at[src, rows]
        return pltpu.make_async_remote_copy(
            src_ref=source, dst_ref=refs[a][1].at[blk, rows],
            send_sem=send.at[a, kind], recv_sem=recv.at[a, kind],
            device_id=(dev,), device_id_type=pl.DeviceIdType.MESH)

    started = []

    def go(cp):
        cp.start()
        started.append(cp)

    mine = [pltpu.make_async_copy(refs[a][0], refs[a][1].at[c], local.at[a]) for a in range(2)]
    mine.append(pltpu.make_async_copy(meta_ref.at[c], metaall.at[c], local.at[2]))
    mine.append(pltpu.make_async_copy(bias_ref, biasall.at[me // PLANE], local.at[3]))
    for a in range(2):
        go(copy(a, 0, None, c, 0, xn))
        go(copy(a, 3, None, c, 1, yn))
        go(copy(a, 1, None, c, 1, xn))
        go(copy(a, 2, None, c, 0, yn))
    for k, peer in enumerate(plane_peers):
        go(pltpu.make_async_remote_copy(
            src_ref=meta_ref.at[peer - base], dst_ref=metaall.at[c], send_sem=msend.at[k],
            recv_sem=mrecv.at[k], device_id=(peer,), device_id_type=pl.DeviceIdType.MESH))
    for k, peer in enumerate(col_peers):
        go(pltpu.make_async_remote_copy(
            src_ref=bias_ref, dst_ref=biasall.at[me // PLANE], send_sem=bsend.at[k],
            recv_sem=brecv.at[k], device_id=(peer,), device_id_type=pl.DeviceIdType.MESH))
    for m in mine:
        m.start()
    for a in range(2):
        go(copy(a, 6, None, c, 0, partner))
        go(copy(a, 7, None, c, 1, partner))

    def arrived(a, kind, blk, h):
        copy(a, kind, blk, blk, h, partner).wait_recv()

    for a in range(2):
        arrived(a, 0, cx, 0)
        go(copy(a, 4, cx, cx, 0, yn))
        go(copy(a, 8, cx, cx, 0, partner))
        arrived(a, 3, cy, 1)
        go(copy(a, 5, cy, cy, 1, xn))
        go(copy(a, 11, cy, cy, 1, partner))
        arrived(a, 1, cx, 1)
        go(copy(a, 9, cx, cx, 1, partner))
        arrived(a, 2, cy, 0)
        go(copy(a, 10, cy, cy, 0, partner))
    for a in range(2):
        arrived(a, 4, cd, 0)
        go(copy(a, 12, cd, cd, 0, partner))
        arrived(a, 5, cd, 1)
        go(copy(a, 13, cd, cd, 1, partner))
    flip = partner - me
    for a in range(2):
        for n, blk in enumerate((c, cx, cy, cd)):
            for h in range(2):
                arrived(a, 6 + 2 * n + h, blk + flip, h)
    for k, peer in enumerate(plane_peers):
        pltpu.make_async_remote_copy(
            src_ref=meta_ref.at[c], dst_ref=metaall.at[(c + PLANE - k - 1) % PLANE], send_sem=msend.at[k],
            recv_sem=mrecv.at[k], device_id=(peer,), device_id_type=pl.DeviceIdType.MESH).wait_recv()
    for k, peer in enumerate(col_peers):
        pltpu.make_async_remote_copy(
            src_ref=bias_ref, dst_ref=biasall.at[(me // PLANE + DEPTH - k - 1) % DEPTH], send_sem=bsend.at[k],
            recv_sem=brecv.at[k], device_id=(peer,), device_id_type=pl.DeviceIdType.MESH).wait_recv()
    for cp in started:
        cp.wait_send()
    for m in mine:
        m.wait()


def gather_call(world, x, dy, meta, bias):
    tok, d = x.shape
    any_spec = pl.BlockSpec(memory_space=pl.ANY)
    vmem = pl.BlockSpec(memory_space=pltpu.VMEM)
    blocks = jax.ShapeDtypeStruct((PLANE, tok, d), x.dtype)
    dma = pltpu.SemaphoreType.DMA
    return pl.pallas_call(
        functools.partial(gather_kernel, world),
        in_specs=[vmem] * 4,
        out_specs=[any_spec] * 4,
        out_shape=[blocks, blocks, jax.ShapeDtypeStruct(meta.shape, F32),
                   jax.ShapeDtypeStruct((DEPTH,) + bias.shape, F32)],
        scratch_shapes=[dma((2, 14)), dma((2, 14)), dma((PLANE - 1,)), dma((PLANE - 1,)),
                        dma((DEPTH - 1,)), dma((DEPTH - 1,)), dma((4,))],
        compiler_params=pltpu.CompilerParams(collective_id=0, has_side_effects=True, vmem_limit_bytes=24 * 2**20),
        cost_estimate=pl.CostEstimate(flops=100 * 10**9, bytes_accessed=40 * 2**20, transcendentals=0),
        name="plane_gather",
    )(x, dy, meta, bias)


def rows_kernel(cap, meta_ref, x_ref, dy_ref, xr_ref, qr_ref):
    tok = x_ref.shape[1]
    slot_iota = lax.broadcasted_iota(jnp.int32, (cap, tok), 0).astype(F32)
    for e in range(DEPTH):
        hit = meta_ref[0, e:e + 1, :] == slot_iota
        sel = jnp.where(hit, 1.0, 0.0).astype(BF16)
        w_row = jnp.sum(jnp.where(hit, meta_ref[0, DEPTH + e:DEPTH + e + 1, :], 0.0), axis=1, keepdims=True)
        xr_ref[e] = dot(sel, x_ref[0]).astype(BF16)
        qr_ref[e] = (w_row * dot(sel, dy_ref[0])).astype(BF16)


def rows_call(meta, x_all, dy_all, cap):
    srcs, tok, d = x_all.shape
    tok_spec = pl.BlockSpec((1, tok, d), lambda s: (s, 0, 0))
    row_spec = pl.BlockSpec((DEPTH, cap, d), lambda s: (0, s, 0))
    row_shape = jax.ShapeDtypeStruct((DEPTH, srcs * cap, d), BF16)
    return pl.pallas_call(
        functools.partial(rows_kernel, cap),
        grid=(srcs,),
        in_specs=[pl.BlockSpec((1, 2 * DEPTH, tok), lambda s: (s, 0, 0)), tok_spec, tok_spec],
        out_specs=[row_spec, row_spec],
        out_shape=[row_shape, row_shape],
        compiler_params=pltpu.CompilerParams(dimension_semantics=("arbitrary",), vmem_limit_bytes=VMEM_LIMIT),
        cost_estimate=pl.CostEstimate(flops=4 * srcs * DEPTH * cap * d * tok, bytes_accessed=90 * 2**20, transcendentals=0),
        name="rows",
    )(meta, x_all, dy_all)


def swiglu_parts(h, ff):
    gate_in = h[:, :ff]
    up_in = h[:, ff:]
    g = jnp.minimum(gate_in, LIMIT)
    u1 = jnp.clip(up_in, -LIMIT, LIMIT) + 1.0
    sg = 1.0 / (1.0 + jnp.exp(-ALPHA * g))
    return gate_in, up_in, u1, sg, g * sg


def down_kernel(ff, xr_ref, qr_ref, wgu_ref, bgu_ref, act_ref, dwd_ref):
    h = dot(xr_ref[0], wgu_ref[0]) + bgu_ref[0]
    _, _, u1, _, gs = swiglu_parts(h, ff)
    act = (gs * u1).astype(BF16)
    act_ref[0] = act
    q = qr_ref[0]
    dwd = dot(act, q, ((0,), (0,)))
    dbd = jnp.broadcast_to(jnp.sum(q.astype(F32), axis=0, keepdims=True), (8, q.shape[1]))
    step = pl.program_id(1)

    @pl.when(step == 0)
    def _():
        dwd_ref[0, :ff] = dwd
        dwd_ref[0, ff:] = dbd

    @pl.when(step > 0)
    def _():
        dwd_ref[0, :ff] += dwd
        dwd_ref[0, ff:] += dbd


def down_call(x_rows, q_rows, wgu, bgu, tile):
    experts, rows, d = x_rows.shape
    ff2 = wgu.shape[2]
    ff = ff2 // 2
    per_e = lambda a, b: pl.BlockSpec((1, a, b), lambda e, s: (e, 0, 0))
    row_spec = pl.BlockSpec((1, tile, d), lambda e, s: (e, s, 0))
    return pl.pallas_call(
        functools.partial(down_kernel, ff),
        grid=(experts, rows // tile),
        in_specs=[row_spec, row_spec, per_e(d, ff2), per_e(1, ff2)],
        out_specs=[pl.BlockSpec((1, tile, ff), lambda e, s: (e, s, 0)), per_e(ff + 8, d)],
        out_shape=[jax.ShapeDtypeStruct((experts, rows, ff), BF16),
                   jax.ShapeDtypeStruct((experts, ff + 8, d), F32)],
        compiler_params=pltpu.CompilerParams(dimension_semantics=("arbitrary", "arbitrary"), vmem_limit_bytes=VMEM_LIMIT),
        cost_estimate=pl.CostEstimate(flops=3 * experts * rows * d * ff2, bytes_accessed=80 * 2**20, transcendentals=0),
        name="down_grad",
    )(x_rows, q_rows, wgu, bgu)


def up_kernel(ff, cap, meta_ref, dy_ref, xr_ref, qr_ref, act_ref, wgu_ref, wd_ref, bgu_ref, bd_ref,
              y_ref, p_ref, dwgu_ref, r_ref, dhs):
    tile = xr_ref.shape[1]
    half = tile // 2
    for i in range(2):
        rows = pl.ds(i * half, half)
        h = dot(xr_ref[0, rows, :], wgu_ref[0]) + bgu_ref[0]
        gate_in, up_in, u1, sg, gs = swiglu_parts(h, ff)
        da = dot(qr_ref[0, rows, :], wd_ref[0], ((1,), (1,)))
        pass_g = jnp.where(gate_in < LIMIT, 1.0, jnp.where(gate_in == LIMIT, 0.5, 0.0))
        up_abs = jnp.abs(up_in)
        pass_u = jnp.where(up_abs < LIMIT, 1.0, jnp.where(up_abs == LIMIT, 0.5, 0.0))
        dhs[rows, :ff] = ((da * u1) * (sg + ALPHA * gs * (1.0 - sg)) * pass_g).astype(BF16)
        dhs[rows, ff:] = (da * gs * pass_u).astype(BF16)
        p_ref[0, rows, :] = dot(dhs[rows, :], wgu_ref[0], ((1,), (1,))).astype(BF16)
        y_ref[0, rows, :] = (dot(act_ref[0, rows, :], wd_ref[0]) + bd_ref[0]).astype(BF16)
    dh = dhs[...]
    dwgu = dot(xr_ref[0], dh, ((0,), (0,)))
    d = dwgu.shape[0]
    dbgu = jnp.broadcast_to(jnp.sum(dh.astype(F32), axis=0, keepdims=True), (8, 2 * ff))
    step = pl.program_id(1)

    @pl.when(step == 0)
    def _():
        dwgu_ref[0, :d] = dwgu
        dwgu_ref[0, d:] = dbgu

    @pl.when(step > 0)
    def _():
        dwgu_ref[0, :d] += dwgu
        dwgu_ref[0, d:] += dbgu


def up_call(x_rows, q_rows, act, wgu, wd, bgu, bd, tile):
    experts, rows, d = x_rows.shape
    ff2 = wgu.shape[2]
    ff = ff2 // 2
    per_e = lambda a, b: pl.BlockSpec((1, a, b), lambda e, s: (e, 0, 0))
    row_spec = pl.BlockSpec((1, tile, d), lambda e, s: (e, s, 0))
    row_shape = jax.ShapeDtypeStruct((experts, rows, d), BF16)

    def body(xr, qr, a, w1, w2, b1, b2, y, p, dw, dhs):
        up_kernel(ff, 0, None, None, xr, qr, a, w1, w2, b1, b2, y, p, dw, None, dhs)

    return pl.pallas_call(
        body,
        grid=(experts, rows // tile),
        in_specs=[row_spec, row_spec, pl.BlockSpec((1, tile, ff), lambda e, s: (e, s, 0)),
                  per_e(d, ff2), per_e(ff, d), per_e(1, ff2), per_e(1, d)],
        out_specs=[row_spec, row_spec, per_e(d + 8, ff2)],
        out_shape=[row_shape, row_shape, jax.ShapeDtypeStruct((experts, d + 8, ff2), F32)],
        scratch_shapes=[pltpu.VMEM((tile, ff2), BF16)],
        compiler_params=pltpu.CompilerParams(dimension_semantics=("arbitrary", "arbitrary"), vmem_limit_bytes=VMEM_LIMIT),
        cost_estimate=pl.CostEstimate(flops=8 * experts * rows * d * ff2, bytes_accessed=140 * 2**20, transcendentals=0),
        name="up_grad",
    )(x_rows, q_rows, act, wgu, wd, bgu, bd)


def combine_kernel(cap, chunk, meta_ref, dy_hbm, y_hbm, p_hbm, out_ref, dx_ref, r_ref, core_in, link_in,
                   stage, ybuf, pbuf, dybuf, ysem, psem, dysem, csend, crecv, lsend, lrecv, loads):
    me = lax.axis_index('ep')
    c, partner, xn, yn = place(me)
    base = me - c
    core, xb, yb = c % 2, (c // 2) % 2, c // 4
    half = out_ref.shape[0] // 2
    d = out_ref.shape[1]

    barrier = pltpu.get_barrier_semaphore()
    for peer in (partner, xn, yn):
        pl.semaphore_signal(barrier, inc=1, device_id=(peer,), device_id_type=pl.DeviceIdType.MESH)
    pl.semaphore_wait(barrier, 3)

    def where(t):
        u, mine = t // 2, t % 2
        v, i = u // 2, u % 2
        diag = 1 - (v + 3) // 4
        side = ((v + 1) // 2) % 2
        isx, isy = diag + side * (1 - i), diag + side * i
        swap = (v // 2) * (1 - v // 3)
        h = i + swap * (1 - 2 * i)
        dest = c + isx * (2 - 4 * xb) + isy * (4 - 8 * yb) + (1 - mine) * (1 - 2 * core)
        slot = mine * (u % 6) + (1 - mine) * (6 + u % 2)
        return dest, h, mine, slot

    def fetch(t):
        dest, h, _, _ = where(t)
        b = t % 2
        return (pltpu.make_async_copy(y_hbm.at[:, pl.ds(dest * cap, cap), :], ybuf.at[b], ysem.at[b]),
                pltpu.make_async_copy(p_hbm.at[:, pl.ds(dest * cap, cap), :], pbuf.at[b], psem.at[b]),
                pltpu.make_async_copy(dy_hbm.at[dest, pl.ds(h * half, half), :], dybuf.at[b], dysem.at[b]))

    def to_core(u):
        return pltpu.make_async_remote_copy(
            src_ref=stage.at[6 + u % 2], dst_ref=core_in.at[u], send_sem=csend.at[u], recv_sem=crecv.at[u],
            device_id=(partner,), device_id_type=pl.DeviceIdType.MESH)

    def to_link(u):
        return pltpu.make_async_remote_copy(
            src_ref=stage.at[u], dst_ref=link_in.at[u], send_sem=lsend.at[u], recv_sem=lrecv.at[u],
            device_id=((xn, yn, xn, yn, xn, yn)[u],), device_id_type=pl.DeviceIdType.MESH)

    def load(src, slot, s):
        cp = pltpu.make_async_copy(src, stage.at[slot], loads.at[s])
        cp.start()
        return cp

    def add_into(slot, other):
        @pl.loop(0, half // chunk)
        def _(k):
            rows = pl.ds(pl.multiple_of(k * chunk, chunk), chunk)
            stage[slot, 0, rows, :] += stage[other, 0, rows, :]
            stage[slot, 1, rows, :] += stage[other, 1, rows, :]

    def before(t):
        u, mine = t // 2, t % 2
        if mine:
            to_core(u).wait_recv()
            load(core_in.at[u], u % 6, 0).wait()
            if u in (4, 5):
                other = 5 - u
                to_link(other).wait_recv()
                to_link(other).wait_send()
                load(link_in.at[other], other, 1).wait()
                add_into(u, other)
        elif u >= 2:
            to_core(u - 2).wait_send()

    def after(t):
        u, mine = t // 2, t % 2
        if not mine:
            to_core(u).start()
        elif u < 6:
            to_link(u).start()

    for cp in fetch(0):
        cp.start()
    slot_iota = lax.broadcasted_iota(jnp.int32, (chunk, cap), 1).astype(F32)
    lane = lax.broadcasted_iota(jnp.int32, (chunk, 8), 1)

    @pl.loop(0, 16)
    def _(t):
        dest, h, mine, slot = where(t)
        b = t % 2
        for cp in fetch(t):
            cp.wait()

        @pl.when(t < 15)
        def _():
            for cp in fetch(t + 1):
                cp.start()

        for k in range(16):
            @pl.when(t == k)
            def _():
                before(k)

        @pl.loop(0, half // chunk)
        def _(k):
            rows = pl.ds(pl.multiple_of(k * chunk, chunk), chunk)
            tokens = pl.ds(pl.multiple_of(h * half + k * chunk, chunk), chunk)
            meta = meta_ref[dest, tokens, :]
            dy = dybuf[b, rows, :].astype(F32)
            out = jnp.zeros((chunk, d), F32)
            dx = jnp.zeros((chunk, d), F32)
            r = jnp.zeros((chunk, 8), F32)
            for j in range(DEPTH):
                sel = jnp.where(meta[:, j:j + 1] == slot_iota, 1.0, 0.0).astype(BF16)
                y = dot(sel, ybuf[b, j])
                out += meta[:, DEPTH + j:DEPTH + j + 1] * y
                r = jnp.where(lane == j, jnp.sum(dy * y, axis=1, keepdims=True), r)
                dx += dot(sel, pbuf[b, j])
            r_ref[dest, tokens, :] = r

            @pl.when(mine == 0)
            def _():
                stage[slot, 0, rows, :] = out
                stage[slot, 1, rows, :] = dx

            @pl.when(mine == 1)
            def _():
                stage[slot, 0, rows, :] += out
                stage[slot, 1, rows, :] += dx

        for k in range(16):
            @pl.when(t == k)
            def _():
                after(k)

    for slot, (first, second) in ((0, (2, 5)), (1, (4, 3))):
        for n in (first, second):
            to_link(n).wait_recv()
            to_link(n).wait_send()
            load(link_in.at[n], n, 1).wait()
            add_into(slot, n)
        out_ref[pl.ds(slot * half, half), :] = stage[slot, 0].astype(BF16)
        dx_ref[pl.ds(slot * half, half), :] = stage[slot, 1]
    to_core(6).wait_send()
    to_core(7).wait_send()


def combine_call(meta_t, dy_all, y_rows, p_rows, cap):
    srcs, tok, d = dy_all.shape
    half = tok // 2
    any_spec = pl.BlockSpec(memory_space=pl.ANY)
    vmem = pl.BlockSpec(memory_space=pltpu.VMEM)
    dma = pltpu.SemaphoreType.DMA
    chunk = min(128, half)
    return pl.pallas_call(
        functools.partial(combine_kernel, cap, chunk),
        in_specs=[vmem, any_spec, any_spec, any_spec],
        out_specs=[vmem, vmem, vmem, any_spec, any_spec],
        out_shape=[jax.ShapeDtypeStruct((tok, d), BF16), jax.ShapeDtypeStruct((tok, d), F32),
                   jax.ShapeDtypeStruct((srcs, tok, 8), F32),
                   jax.ShapeDtypeStruct((8, 2, half, d), F32), jax.ShapeDtypeStruct((6, 2, half, d), F32)],
        scratch_shapes=[pltpu.VMEM((8, 2, half, d), F32),
                        pltpu.VMEM((2, DEPTH, cap, d), BF16), pltpu.VMEM((2, DEPTH, cap, d), BF16),
                        pltpu.VMEM((2, half, d), BF16),
                        dma((2,)), dma((2,)), dma((2,)), dma((8,)), dma((8,)), dma((6,)), dma((6,)), dma((2,))],
        compiler_params=pltpu.CompilerParams(collective_id=1, has_side_effects=True, vmem_limit_bytes=67043328),
        cost_estimate=pl.CostEstimate(flops=300 * 10**9, bytes_accessed=300 * 2**20, transcendentals=0),
        name="combine_scatter",
    )(meta_t, dy_all, y_rows, p_rows)


def solution(mesh):
    world = mesh.shape['ep']
    plane_groups = [[PLANE * z + c for c in range(PLANE)] for z in range(DEPTH)]
    col_groups = [[PLANE * z + c for z in range(DEPTH)] for c in range(PLANE)]

    def local_block(hidden, grad_out, w_router, b_router, expert_ids, slot_ids, w_gate_up, b_gate_up, w_down, b_down):
        tok, d = hidden.shape
        top_k = expert_ids.shape[1]
        experts = w_router.shape[1]
        ff = w_down.shape[1]
        cap = (3 * tok * top_k + 2 * experts - 1) // (2 * experts)

        ids = jnp.arange(experts, dtype=jnp.int32)
        match = expert_ids[:, :, None] == ids
        chosen = jnp.any(match, axis=1)
        slot = jnp.max(jnp.where(match, slot_ids[:, :, None], -1), axis=1)
        logits = jnp.dot(hidden, w_router, preferred_element_type=F32) + b_router
        peak = jnp.max(jnp.where(chosen, logits, -jnp.inf), axis=1, keepdims=True)
        expd = jnp.where(chosen, jnp.exp(jnp.where(chosen, logits, peak) - peak), 0.0)
        gate = expd / jnp.sum(expd, axis=1, keepdims=True)
        meta = jnp.concatenate([slot.astype(F32).reshape(tok, DEPTH, PLANE), gate.reshape(tok, DEPTH, PLANE)], axis=1)

        col = jnp.arange(2 * ff, dtype=jnp.int32)
        perm = (col[:, None] == jnp.where(col < ff, 2 * col, 2 * (col - ff) + 1)[None, :]).astype(BF16)
        wgu = jnp.dot(w_gate_up[0], perm, preferred_element_type=F32).astype(BF16)
        bgu = b_gate_up.reshape(ff, 2).T.reshape(1, 2 * ff)
        w_cat = lax.all_gather(jnp.concatenate([wgu, w_down[0]], axis=0), 'ep', axis_index_groups=col_groups)
        bias = jnp.concatenate([bgu, b_down, jnp.zeros((6, d), F32)], axis=0)
        x_all, dy_all, meta_r, b_cat = gather_call(world, hidden, grad_out, meta.transpose(2, 1, 0), bias)
        meta_t = meta_r.transpose(0, 2, 1)
        wgu_all, wd_all, bgu_all, bd_all = w_cat[:, :d], w_cat[:, d:], b_cat[:, :1], b_cat[:, 1:2]

        x_rows, q_rows = rows_call(meta_r, x_all, dy_all, cap)
        act, dwd = down_call(x_rows, q_rows, wgu_all, bgu_all, 2 * cap)
        y_rows, p_rows, dwgu = up_call(x_rows, q_rows, act, wgu_all, wd_all, bgu_all, bd_all, 2 * cap)
        block_out, dx, r_part, _, _ = combine_call(meta_t, dy_all, y_rows, p_rows, cap)

        scatter = functools.partial(lax.psum_scatter, axis_name='ep', scatter_dimension=0, tiled=True)
        grad_wd = scatter(dwd, axis_index_groups=col_groups)
        grad_wgu = scatter(dwgu, axis_index_groups=col_groups)

        r = lax.all_to_all(r_part[:, :, :DEPTH], 'ep', 0, 0, tiled=True, axis_index_groups=plane_groups)
        r = r.transpose(1, 2, 0).reshape(tok, experts)
        sel_grad = gate * (r - jnp.sum(gate * r, axis=1, keepdims=True))
        logit_grad = sel_grad.astype(BF16)
        router_dx = lax.dot_general(logit_grad, w_router, (((1,), (1,)), ((), ())), preferred_element_type=F32)
        grad_hidden = (dx + router_dx).astype(BF16)
        grad_w_router = lax.psum(lax.dot_general(hidden, logit_grad, (((0,), (0,)), ((), ())), preferred_element_type=F32), 'ep')
        grad_b_router = lax.psum(jnp.sum(logit_grad.astype(F32), axis=0), 'ep')

        grad_w_gate_up = jnp.stack([grad_wgu[0, :d, :ff], grad_wgu[0, :d, ff:]], axis=-1).reshape(1, d, 2 * ff)
        grad_b_gate_up = grad_wgu[0, d].reshape(2, ff).T.reshape(1, 2 * ff)
        return (block_out, grad_hidden, grad_w_router, grad_b_router, grad_w_gate_up,
                grad_b_gate_up, grad_wd[:, :ff], grad_wd[:, ff])

    tok_spec = P('ep', None)
    in_specs = (tok_spec, tok_spec, P(None, None), P(None), tok_spec, tok_spec, P('ep', None, None), P('ep', None), P('ep', None, None), P('ep', None))
    out_specs = (tok_spec, tok_spec, P(None, None), P(None), P('ep', None, None), P('ep', None), P('ep', None, None), P('ep', None))
    return jax.shard_map(local_block, mesh=mesh, in_specs=in_specs, out_specs=out_specs, check_vma=False)
```

```python
import functools

import jax
import jax.numpy as jnp
from jax import lax
from jax.experimental import pallas as pl
from jax.experimental.layout import Layout, with_layout_constraint
from jax.experimental.pallas import tpu as pltpu
from jax.sharding import PartitionSpec as P

LIMIT = 7.0
ALPHA = 1.702
F32 = jnp.float32
BF16 = jnp.bfloat16
PLANE = 8
DEPTH = 4
VMEM_LIMIT = 62 * 1024 * 1024


def dot(a, b, dims=((1,), (0,))):
    return lax.dot_general(a, b, (dims, ((), ())), preferred_element_type=F32)


def cost(gflops, mib):
    return pl.CostEstimate(flops=gflops * 10**9, bytes_accessed=mib * 2**20, transcendentals=0)


def place(me):
    c = me % PLANE
    core, xb, yb = c % 2, (c // 2) % 2, c // 4
    return c, me + 1 - 2 * core, me + 2 - 4 * xb, me + 4 - 8 * yb


def gather_kernel(world, cap, x_ref, dy_ref, meta_ref, bias_ref, xall, dyall, metaall, biasall, xr_hbm, qr_hbm,
                  xbuf, dybuf, xst, qst, send, recv, msend, mrecv, bsend, brecv, local, ld, st):
    me = lax.axis_index('ep')
    c, partner, xn, yn = place(me)
    base = me - c
    plane_peers = [base + (c + k) % PLANE for k in range(1, PLANE)]
    col_peers = [(me + PLANE * k) % world for k in range(1, DEPTH)]
    cx, cy, flip = xn - base, yn - base, partner - me
    cd = cx + cy - c
    half = x_ref.shape[0] // 2

    barrier = pltpu.get_barrier_semaphore()
    for peer in plane_peers + col_peers:
        pl.semaphore_signal(barrier, inc=1, device_id=(peer,), device_id_type=pl.DeviceIdType.MESH)
    pl.semaphore_wait(barrier, len(plane_peers) + len(col_peers))

    refs = ((x_ref, xall), (dy_ref, dyall))

    def hop(a, kind, arriving=False):
        if kind < 6:
            h = (0, 1, 0, 1, 0, 1)[kind]
            dev = (xn, xn, yn, yn, yn, xn)[kind]
            blk = (None, None, None, None, cx, cy)[kind]
        else:
            h, dev = kind % 2, partner
            blk = (None, cx, cy, cd)[(kind - 6) // 2]
        rows = pl.ds(h * half, half)
        source = refs[a][0].at[rows] if blk is None else refs[a][1].at[blk, rows]
        into = c if blk is None else blk
        if arriving:
            into = (cx, cx, cy, cy, cd, cd)[kind] if kind < 6 else into + flip
        return pltpu.make_async_remote_copy(
            src_ref=source, dst_ref=refs[a][1].at[into, rows],
            send_sem=send.at[a, kind], recv_sem=recv.at[a, kind],
            device_id=(dev,), device_id_type=pl.DeviceIdType.MESH)

    def small(k, peer, is_bias, arriving=False):
        if is_bias:
            return pltpu.make_async_remote_copy(
                src_ref=bias_ref, dst_ref=biasall.at[(me // PLANE + (DEPTH - k - 1 if arriving else 0)) % DEPTH],
                send_sem=bsend.at[k],
                recv_sem=brecv.at[k], device_id=(peer,), device_id_type=pl.DeviceIdType.MESH)
        return pltpu.make_async_remote_copy(
            src_ref=meta_ref.at[peer - base], dst_ref=metaall.at[(c + (PLANE - k - 1 if arriving else 0)) % PLANE],
            send_sem=msend.at[k],
            recv_sem=mrecv.at[k], device_id=(peer,), device_id_type=pl.DeviceIdType.MESH)

    smalls = [small(k, peer, False) for k, peer in enumerate(plane_peers)]
    smalls += [small(k, peer, True) for k, peer in enumerate(col_peers)]
    for cp in smalls:
        cp.start()
    for a in range(2):
        for kind in (0, 3, 1, 2):
            hop(a, kind).start()
    for a in range(2):
        for kind in (6, 7):
            hop(a, kind).start()
    bias_own = pltpu.make_async_copy(bias_ref, biasall.at[me // PLANE], local.at[0])
    bias_own.start()
    meta_own = pltpu.make_async_copy(meta_ref.at[c], metaall.at[c], local.at[1])
    meta_own.start()
    dy_own = pltpu.make_async_copy(dybuf.at[0], dyall.at[c], local.at[2])

    def block(t):
        v, f = t // 2, t % 2
        return c + (v % 2) * (cx - c) + (v // 2) * (cy - c) + f * flip

    def store(t):
        s, blk = t % 2, block(t)
        return (pltpu.make_async_copy(xst.at[s], xr_hbm.at[:, pl.ds(blk * cap, cap), :], st.at[0, s]),
                pltpu.make_async_copy(qst.at[s], qr_hbm.at[:, pl.ds(blk * cap, cap), :], st.at[1, s]))

    def arrive(a, kind, *onward):
        hop(a, kind, True).wait_recv()
        for nxt in onward:
            hop(a, nxt).start()

    def before(t):
        if t == 1:
            for n, peer in enumerate(plane_peers):
                small(n, peer, False, True).wait_recv()
            for n, peer in enumerate(col_peers):
                small(n, peer, True, True).wait_recv()
            for a in range(2):
                arrive(a, 6)
                arrive(a, 7)
        if t == 2:
            dy_own.wait()
            for a in range(2):
                arrive(a, 0, 4, 8)
                arrive(a, 3, 5, 11)
                arrive(a, 1, 9)
                arrive(a, 2, 10)
        if t in (3, 5):
            for a in range(2):
                arrive(a, 8 if t == 3 else 10)
                arrive(a, 9 if t == 3 else 11)
        if t == 6:
            for a in range(2):
                arrive(a, 4, 12)
                arrive(a, 5, 13)
        if t == 7:
            for a in range(2):
                arrive(a, 12)
                arrive(a, 13)
        s = t % 2
        blk = block(t)
        sources = (x_ref, dy_ref) if t == 0 else (xall.at[blk], dyall.at[blk])
        loads = [pltpu.make_async_copy(sources[0], xbuf.at[s], ld.at[0]),
                 pltpu.make_async_copy(sources[1], dybuf.at[s], ld.at[1])]
        for cp in loads:
            cp.start()
        for cp in loads:
            cp.wait()
        if t == 0:
            dy_own.start()
            meta_own.wait()

    slot_iota = lax.broadcasted_iota(jnp.int32, (cap, 2 * half), 0).astype(F32)

    @pl.loop(0, PLANE)
    def _(t):
        s = t % 2
        for k in range(PLANE):
            @pl.when(t == k)
            def _():
                before(k)

        @pl.when(t >= 2)
        def _():
            for cp in store(t - 2):
                cp.wait()

        blk = block(t)
        for e in range(DEPTH):
            hit = metaall[blk, e:e + 1, :] == slot_iota
            sel = jnp.where(hit, 1.0, 0.0).astype(BF16)
            w_row = jnp.sum(jnp.where(hit, metaall[blk, DEPTH + e:DEPTH + e + 1, :], 0.0), axis=1, keepdims=True)
            xst[s, e] = dot(sel, xbuf[s]).astype(BF16)
            qst[s, e] = (w_row * dot(sel, dybuf[s])).astype(BF16)
        for cp in store(t):
            cp.start()

    for t in (PLANE - 2, PLANE - 1):
        for cp in store(t):
            cp.wait()
    bias_own.wait()
    for a in range(2):
        for kind in range(14):
            hop(a, kind).wait_send()
    for cp in smalls:
        cp.wait_send()


def gather_call(world, x, dy, meta, bias, cap):
    tok, d = x.shape
    any_spec = pl.BlockSpec(memory_space=pl.ANY)
    vmem = pl.BlockSpec(memory_space=pltpu.VMEM)
    blocks = jax.ShapeDtypeStruct((PLANE, tok, d), x.dtype)
    rows = jax.ShapeDtypeStruct((DEPTH, PLANE * cap, d), BF16)
    dma = pltpu.SemaphoreType.DMA
    hops, seven, three = dma((2, 14)), dma((PLANE - 1,)), dma((DEPTH - 1,))
    return pl.pallas_call(
        functools.partial(gather_kernel, world, cap),
        in_specs=[any_spec, any_spec, vmem, vmem],
        out_specs=[any_spec, any_spec, vmem, any_spec, any_spec, any_spec],
        out_shape=[blocks, blocks, jax.ShapeDtypeStruct(meta.shape, F32),
                   jax.ShapeDtypeStruct((DEPTH,) + bias.shape, F32), rows, rows],
        scratch_shapes=[pltpu.VMEM((2, tok, d), BF16), pltpu.VMEM((2, tok, d), BF16),
                        pltpu.VMEM((2, DEPTH, cap, d), BF16), pltpu.VMEM((2, DEPTH, cap, d), BF16),
                        hops, hops, seven, seven, three, three, three, dma((2,)), dma((2, 2))],
        compiler_params=pltpu.CompilerParams(collective_id=0, has_side_effects=True, vmem_limit_bytes=60 * 2**20),
        cost_estimate=cost(100, 140),
        name="plane_gather",
    )(x, dy, meta, bias)


def swiglu_parts(h, ff):
    gate_in = h[:, :ff]
    up_in = h[:, ff:]
    g = jnp.minimum(gate_in, LIMIT)
    u1 = jnp.clip(up_in, -LIMIT, LIMIT) + 1.0
    sg = 1.0 / (1.0 + jnp.exp(-ALPHA * g))
    return gate_in, up_in, u1, sg, g * sg


def down_kernel(ff, xr_ref, qr_ref, wgu_ref, bgu_ref, act_ref, dwd_ref):
    h = dot(xr_ref[...], wgu_ref[...]) + bgu_ref[...]
    _, _, u1, _, gs = swiglu_parts(h, ff)
    act = (gs * u1).astype(BF16)
    act_ref[...] = act
    q = qr_ref[...]
    dwd = dot(act, q, ((0,), (0,)))
    dbd = jnp.broadcast_to(jnp.sum(q.astype(F32), axis=0, keepdims=True), (8, q.shape[1]))
    step = pl.program_id(1)

    @pl.when(step == 0)
    def _():
        dwd_ref[:ff] = dwd
        dwd_ref[ff:] = dbd

    @pl.when(step > 0)
    def _():
        dwd_ref[:ff] += dwd
        dwd_ref[ff:] += dbd


def down_call(x_rows, q_rows, wgu, bgu, tile):
    experts, rows, d = x_rows.shape
    ff2 = wgu.shape[2]
    ff = ff2 // 2
    per_e = lambda a, b: pl.BlockSpec((None, a, b), lambda e, s: (e, 0, 0))
    row_spec = pl.BlockSpec((None, tile, d), lambda e, s: (e, s, 0))
    return pl.pallas_call(
        functools.partial(down_kernel, ff),
        grid=(experts, rows // tile),
        in_specs=[row_spec, row_spec, per_e(d, ff2), per_e(1, ff2)],
        out_specs=[pl.BlockSpec((None, tile, ff), lambda e, s: (e, s, 0)), per_e(ff + 8, d)],
        out_shape=[jax.ShapeDtypeStruct((experts, rows, ff), BF16),
                   jax.ShapeDtypeStruct((experts, ff + 8, d), F32)],
        compiler_params=pltpu.CompilerParams(dimension_semantics=("arbitrary", "arbitrary"), vmem_limit_bytes=VMEM_LIMIT),
        cost_estimate=cost(39, 80),
        name="down_grad",
    )(x_rows, q_rows, wgu, bgu)


def up_kernel(ff, xr_ref, qr_ref, act_ref, wgu_ref, wd_ref, bgu_ref, bd_ref,
              y_ref, p_ref, dwgu_ref, dhs):
    tile = xr_ref.shape[0]
    half = tile // 2
    for i in range(2):
        rows = pl.ds(i * half, half)
        h = dot(xr_ref[rows, :], wgu_ref[...]) + bgu_ref[...]
        gate_in, up_in, u1, sg, gs = swiglu_parts(h, ff)
        da = dot(qr_ref[rows, :], wd_ref[...], ((1,), (1,)))
        pass_g = jnp.where(gate_in < LIMIT, 1.0, jnp.where(gate_in == LIMIT, 0.5, 0.0))
        up_abs = jnp.abs(up_in)
        pass_u = jnp.where(up_abs < LIMIT, 1.0, jnp.where(up_abs == LIMIT, 0.5, 0.0))
        dhs[rows, :ff] = ((da * u1) * (sg + ALPHA * gs * (1.0 - sg)) * pass_g).astype(BF16)
        dhs[rows, ff:] = (da * gs * pass_u).astype(BF16)
        p_ref[rows, :] = dot(dhs[rows, :], wgu_ref[...], ((1,), (1,))).astype(BF16)
        y_ref[rows, :] = (dot(act_ref[rows, :], wd_ref[...]) + bd_ref[...]).astype(BF16)
    dh = dhs[...]
    dwgu = dot(xr_ref[...], dh, ((0,), (0,)))
    d = dwgu.shape[0]
    dbgu = jnp.broadcast_to(jnp.sum(dh.astype(F32), axis=0, keepdims=True), (8, 2 * ff))
    step = pl.program_id(1)

    @pl.when(step == 0)
    def _():
        dwgu_ref[:d] = dwgu
        dwgu_ref[d:] = dbgu

    @pl.when(step > 0)
    def _():
        dwgu_ref[:d] += dwgu
        dwgu_ref[d:] += dbgu


def up_call(x_rows, q_rows, act, wgu, wd, bgu, bd, tile):
    experts, rows, d = x_rows.shape
    ff2 = wgu.shape[2]
    ff = ff2 // 2
    per_e = lambda a, b: pl.BlockSpec((None, a, b), lambda e, s: (e, 0, 0))
    row_spec = pl.BlockSpec((None, tile, d), lambda e, s: (e, s, 0))
    row_shape = jax.ShapeDtypeStruct((experts, rows, d), BF16)

    return pl.pallas_call(
        functools.partial(up_kernel, ff),
        grid=(experts, rows // tile),
        in_specs=[row_spec, row_spec, pl.BlockSpec((None, tile, ff), lambda e, s: (e, s, 0)),
                  per_e(d, ff2), per_e(ff, d), per_e(1, ff2), per_e(1, d)],
        out_specs=[row_spec, row_spec, per_e(d + 8, ff2)],
        out_shape=[row_shape, row_shape, jax.ShapeDtypeStruct((experts, d + 8, ff2), F32)],
        scratch_shapes=[pltpu.VMEM((tile, ff2), BF16)],
        compiler_params=pltpu.CompilerParams(dimension_semantics=("arbitrary", "arbitrary"), vmem_limit_bytes=VMEM_LIMIT),
        cost_estimate=cost(103, 140),
        name="up_grad",
    )(x_rows, q_rows, act, wgu, wd, bgu, bd)


def combine_kernel(cap, chunk, world, meta_ref, dy_hbm, y_hbm, p_hbm, gate_ref, wr_ref, hid_ref,
                   out_ref, dx_ref, fin_ref, core_in, link_in,
                   stage, ybuf, pbuf, dybuf, r_rows, r_in, dw, dw_in, dz_in, dz,
                   ysem, psem, dysem, csend, crecv, lsend, lrecv, loads,
                   rsend, rrecv, wsend, wrecv, zsend, zrecv, fsend, frecv):
    me = lax.axis_index('ep')
    c, partner, xn, yn = place(me)
    base = me - c
    core, xb, yb = c % 2, (c // 2) % 2, c // 4
    half = out_ref.shape[0] // 2
    d = out_ref.shape[1]

    barrier = pltpu.get_barrier_semaphore()
    plane_peers = [base + (c + k) % PLANE for k in range(1, PLANE)]
    col_peers = [(me + PLANE * k) % world for k in range(1, DEPTH)]
    for peer in plane_peers + col_peers:
        pl.semaphore_signal(barrier, inc=1, device_id=(peer,), device_id_type=pl.DeviceIdType.MESH)
    pl.semaphore_wait(barrier, len(plane_peers) + len(col_peers))

    def exchange(peers, source, into, at, ssem, rsem, arriving=False):
        count = len(peers) + 1
        return [pltpu.make_async_remote_copy(
            src_ref=source(peer), dst_ref=into.at[(at + (count - k - 1 if arriving else 0)) % count],
            send_sem=ssem.at[k], recv_sem=rsem.at[k],
            device_id=(peer,), device_id_type=pl.DeviceIdType.MESH) for k, peer in enumerate(peers)]

    def begin(*how):
        cps = exchange(*how)
        for cp in cps:
            cp.start()
        return how, cps

    def finish(begun):
        for cp in exchange(*begun[0], arriving=True):
            cp.wait_recv()

    def where(t):
        u, mine = t // 2, t % 2
        v, i = u // 2, u % 2
        diag = 1 - (v + 3) // 4
        side = ((v + 1) // 2) % 2
        isx, isy = diag + side * (1 - i), diag + side * i
        swap = (v // 2) * (1 - v // 3)
        h = i + swap * (1 - 2 * i)
        dest = c + isx * (2 - 4 * xb) + isy * (4 - 8 * yb) + (1 - mine) * (1 - 2 * core)
        slot = mine * (u % 6) + (1 - mine) * (6 + u % 2)
        return dest, h, mine, slot

    def fetch(t):
        dest, h, _, _ = where(t)
        b = t % 2
        return (pltpu.make_async_copy(y_hbm.at[:, pl.ds(dest * cap, cap), :], ybuf.at[b], ysem.at[b]),
                pltpu.make_async_copy(p_hbm.at[:, pl.ds(dest * cap, cap), :], pbuf.at[b], psem.at[b]),
                pltpu.make_async_copy(dy_hbm.at[dest, pl.ds(h * half, half), :], dybuf.at[b], dysem.at[b]))

    def to_core(u):
        return pltpu.make_async_remote_copy(
            src_ref=stage.at[6 + u % 2], dst_ref=core_in.at[u], send_sem=csend.at[u], recv_sem=crecv.at[u],
            device_id=(partner,), device_id_type=pl.DeviceIdType.MESH)

    def to_link(u):
        return pltpu.make_async_remote_copy(
            src_ref=stage.at[u], dst_ref=link_in.at[u], send_sem=lsend.at[u], recv_sem=lrecv.at[u],
            device_id=((xn, yn, xn, yn, xn, yn)[u],), device_id_type=pl.DeviceIdType.MESH)

    def load(src, slot, s):
        cp = pltpu.make_async_copy(src, stage.at[slot], loads.at[s])
        cp.start()
        return cp

    def add_into(slot, other):
        @pl.loop(0, half // chunk)
        def _(k):
            rows = pl.ds(pl.multiple_of(k * chunk, chunk), chunk)
            stage[slot, 0, rows, :] += stage[other, 0, rows, :]
            stage[slot, 1, rows, :] += stage[other, 1, rows, :]

    def before(t):
        u, mine = t // 2, t % 2
        if mine:
            to_core(u).wait_recv()
            load(core_in.at[u], u % 6, 0).wait()
            if u in (4, 5):
                other = 5 - u
                to_link(other).wait_recv()
                to_link(other).wait_send()
                load(link_in.at[other], other, 1).wait()
                add_into(u, other)
        elif u >= 2:
            to_core(u - 2).wait_send()

    def after(t):
        u, mine = t // 2, t % 2
        if not mine:
            to_core(u).start()
        elif u < 6:
            to_link(u).start()

    for cp in fetch(0):
        cp.start()
    slot_iota = lax.broadcasted_iota(jnp.int32, (chunk, cap), 1).astype(F32)
    lane = lax.broadcasted_iota(jnp.int32, (chunk, 128), 1)

    @pl.loop(0, 16)
    def _(t):
        dest, h, mine, slot = where(t)
        b = t % 2
        for cp in fetch(t):
            cp.wait()

        @pl.when(t < 15)
        def _():
            for cp in fetch(t + 1):
                cp.start()

        for k in range(16):
            @pl.when(t == k)
            def _():
                before(k)

        @pl.loop(0, half // chunk)
        def _(k):
            rows = pl.ds(pl.multiple_of(k * chunk, chunk), chunk)
            tokens = pl.ds(pl.multiple_of(h * half + k * chunk, chunk), chunk)
            meta = meta_ref[dest, tokens, :]
            dy = dybuf[b, rows, :].astype(F32)
            out = jnp.zeros((chunk, d), F32)
            dx = jnp.zeros((chunk, d), F32)
            r = jnp.zeros((chunk, 128), F32)
            for j in range(DEPTH):
                sel = jnp.where(meta[:, j:j + 1] == slot_iota, 1.0, 0.0).astype(BF16)
                y = dot(sel, ybuf[b, j])
                out += meta[:, DEPTH + j:DEPTH + j + 1] * y
                r = jnp.where(lane == j, jnp.sum(dy * y, axis=1, keepdims=True), r)
                dx += dot(sel, pbuf[b, j])
            r_rows[dest, :, tokens] = jnp.transpose(r)[:8, :]

            @pl.when(mine == 0)
            def _():
                stage[slot, 0, rows, :] = out
                stage[slot, 1, rows, :] = dx

            @pl.when(mine == 1)
            def _():
                stage[slot, 0, rows, :] += out
                stage[slot, 1, rows, :] += dx

        for k in range(16):
            @pl.when(t == k)
            def _():
                after(k)

    r_cps = begin(plane_peers, lambda peer: r_rows.at[peer - base], r_in, c, rsend, rrecv)

    for slot, (first, second) in ((0, (2, 5)), (1, (4, 3))):
        for n in (first, second):
            to_link(n).wait_recv()
            to_link(n).wait_send()
            load(link_in.at[n], n, 1).wait()
            add_into(slot, n)
        out_ref[pl.ds(slot * half, half), :] = stage[slot, 0].astype(BF16)

    finish(r_cps)
    r_in[c] = r_rows[c]
    flat = (8 * PLANE, 2 * half)
    gate = gate_ref[...].reshape(flat)
    r_all = r_in[...].reshape(flat)
    mean = jnp.sum(gate * r_all, axis=0, keepdims=True)
    dl = (gate * (r_all - mean)).astype(BF16)
    dw[:, :, :d] = dot(dl, hid_ref[...]).reshape(PLANE, 8, d)
    dbias = jnp.sum(dl.astype(F32), axis=1, keepdims=True)
    dw[:, :, d:] = jnp.broadcast_to(dbias, (8 * PLANE, 128)).reshape(PLANE, 8, 128)
    w_cps = begin(plane_peers, lambda peer: dw.at[peer - base], dw_in, c, wsend, wrecv)
    for slot in range(2):
        part = dot(dl[:, slot * half:(slot + 1) * half], wr_ref[...], ((0,), (0,)))
        dx_ref[pl.ds(slot * half, half), :] = (stage[slot, 1] + part).astype(BF16)
    finish(w_cps)
    dw_in[c] = dw[c]
    dz[...] = jnp.sum(dw_in[...], axis=0)
    z_cps = begin(col_peers, lambda peer: dz, dz_in, me // PLANE, zsend, zrecv)
    finish(z_cps)
    dz_in[me // PLANE] = dz[...]
    fin_ref[c] = (dz_in[0] + dz_in[1]) + (dz_in[2] + dz_in[3])
    f_cps = begin(plane_peers, lambda peer: fin_ref.at[c], fin_ref, c, fsend, frecv)
    finish(f_cps)
    to_core(6).wait_send()
    to_core(7).wait_send()
    for cp in r_cps[1] + w_cps[1] + z_cps[1] + f_cps[1]:
        cp.wait_send()


def combine_call(world, meta_t, dy_all, y_rows, p_rows, gate, w_rows, hidden, cap):
    srcs, tok, d = dy_all.shape
    half = tok // 2
    any_spec = pl.BlockSpec(memory_space=pl.ANY)
    vmem = pl.BlockSpec(memory_space=pltpu.VMEM)
    two, three, six, seven, eight = (pltpu.SemaphoreType.DMA((n,)) for n in (2, 3, 6, 7, 8))
    chunk = min(128, half)
    wide = d + 128
    return pl.pallas_call(
        functools.partial(combine_kernel, cap, chunk, world),
        in_specs=[vmem, any_spec, any_spec, any_spec, vmem, vmem, vmem],
        out_specs=[vmem, vmem, vmem, any_spec, any_spec],
        out_shape=[jax.ShapeDtypeStruct((tok, d), BF16), jax.ShapeDtypeStruct((tok, d), BF16),
                   jax.ShapeDtypeStruct((PLANE, 8, wide), F32),
                   jax.ShapeDtypeStruct((8, 2, half, d), F32), jax.ShapeDtypeStruct((6, 2, half, d), F32)],
        scratch_shapes=[pltpu.VMEM((8, 2, half, d), F32),
                        pltpu.VMEM((2, DEPTH, cap, d), BF16), pltpu.VMEM((2, DEPTH, cap, d), BF16),
                        pltpu.VMEM((2, half, d), BF16),
                        pltpu.VMEM((PLANE, 8, tok), F32), pltpu.VMEM((PLANE, 8, tok), F32),
                        pltpu.VMEM((PLANE, 8, wide), F32), pltpu.VMEM((PLANE, 8, wide), F32),
                        pltpu.VMEM((DEPTH, 8, wide), F32), pltpu.VMEM((8, wide), F32),
                        two, two, two, eight, eight, six, six, two,
                        seven, seven, seven, seven, three, three, seven, seven],
        compiler_params=pltpu.CompilerParams(collective_id=1, has_side_effects=True, vmem_limit_bytes=67043328),
        cost_estimate=cost(300, 300),
        name="combine_scatter",
    )(meta_t, dy_all, y_rows, p_rows, gate, w_rows, hidden)


def interleave_kernel(ff, w_ref, out_ref, bias_ref):
    ff2 = 2 * ff
    src = lax.broadcasted_iota(jnp.int32, (ff2, ff2), 0)
    dst = lax.broadcasted_iota(jnp.int32, (ff2, ff2), 1)
    perm = jnp.where(src == dst // 2 + ff * (dst % 2), 1.0, 0.0).astype(BF16)

    def move(v):
        a = v.astype(BF16)
        rest = v - a.astype(F32)
        b = rest.astype(BF16)
        return dot(a, perm) + (dot(b, perm) + dot((rest - b.astype(F32)).astype(BF16), perm))

    d = out_ref.shape[0]
    out_ref[...] = move(w_ref[:d, :])
    bias_ref[...] = move(w_ref[d:, :])


def interleave_call(w, ff):
    rows, ff2 = w.shape
    return pl.pallas_call(
        functools.partial(interleave_kernel, ff),
        out_shape=[jax.ShapeDtypeStruct((rows - 8, ff2), F32), jax.ShapeDtypeStruct((8, ff2), F32)],
        compiler_params=pltpu.CompilerParams(vmem_limit_bytes=48 * 2**20),
        name="interleave",
    )(w)


def solution(mesh):
    world = mesh.shape['ep']
    plane_groups = [[PLANE * z + c for c in range(PLANE)] for z in range(DEPTH)]
    col_groups = [[PLANE * z + c for z in range(DEPTH)] for c in range(PLANE)]

    def local_block(hidden, grad_out, w_router, b_router, expert_ids, slot_ids, w_gate_up, b_gate_up, w_down, b_down):
        tok, d = hidden.shape
        top_k = expert_ids.shape[1]
        experts = w_router.shape[1]
        ff = w_down.shape[1]
        cap = (3 * tok * top_k + 2 * experts - 1) // (2 * experts)

        ids = jnp.arange(experts, dtype=jnp.int32)
        match = expert_ids[:, :, None] == ids
        chosen = jnp.any(match, axis=1)
        slot = jnp.max(jnp.where(match, slot_ids[:, :, None], -1), axis=1)
        logits = jnp.dot(hidden, w_router, preferred_element_type=F32) + b_router
        peak = jnp.max(jnp.where(chosen, logits, -jnp.inf), axis=1, keepdims=True)
        expd = jnp.where(chosen, jnp.exp(jnp.where(chosen, logits, peak) - peak), 0.0)
        gate = expd / jnp.sum(expd, axis=1, keepdims=True)
        meta = jnp.concatenate([slot.astype(F32).reshape(tok, DEPTH, PLANE), gate.reshape(tok, DEPTH, PLANE)], axis=1)

        col = jnp.arange(2 * ff, dtype=jnp.int32)
        perm = (col[:, None] == jnp.where(col < ff, 2 * col, 2 * (col - ff) + 1)[None, :]).astype(BF16)
        wgu = jnp.dot(w_gate_up[0], perm, preferred_element_type=F32).astype(BF16)
        bgu = b_gate_up.reshape(ff, 2).T.reshape(1, 2 * ff)
        wgu = with_layout_constraint(wgu[None], Layout((0, 1, 2)))
        wgu_all = lax.all_gather(wgu, 'ep', axis_index_groups=col_groups, tiled=True)
        wd_all = lax.all_gather(w_down[0], 'ep', axis_index_groups=col_groups)
        bias = jnp.concatenate([bgu, b_down, jnp.zeros((6, d), F32)], axis=0)
        _, dy_all, meta_r, b_cat, x_rows, q_rows = gather_call(world, hidden, grad_out, meta.transpose(2, 1, 0), bias, cap)
        meta_t = meta_r.transpose(0, 2, 1)
        bgu_all, bd_all = b_cat[:, :1], b_cat[:, 1:2]

        act, dwd = down_call(x_rows, q_rows, wgu_all, bgu_all, 2 * cap)
        y_rows, p_rows, dwgu = up_call(x_rows, q_rows, act, wgu_all, wd_all, bgu_all, bd_all, 2 * cap)
        gate_rows = jnp.pad(gate.T.reshape(DEPTH, PLANE, tok).transpose(1, 0, 2), ((0, 0), (0, 4), (0, 0)))
        w_rows = jnp.pad(w_router.T.reshape(DEPTH, PLANE, d).transpose(1, 0, 2), ((0, 0), (0, 4), (0, 0)))
        block_out, grad_hidden, router, _, _ = combine_call(
            world, meta_t, dy_all, y_rows, p_rows, gate_rows, w_rows.reshape(8 * PLANE, d), hidden, cap)

        scatter = functools.partial(lax.psum_scatter, axis_name='ep', scatter_dimension=0, tiled=True)
        grad_wd = scatter(dwd, axis_index_groups=col_groups)
        grad_wgu = scatter(dwgu, axis_index_groups=col_groups)

        grad_w_router = router[:, :DEPTH, :d].transpose(2, 1, 0).reshape(d, experts)
        grad_b_router = router[:, :DEPTH, d].T.reshape(experts)
        grad_w_gate_up, grad_b_gate_up = interleave_call(grad_wgu[0], ff)
        return (block_out, grad_hidden, grad_w_router, grad_b_router, grad_w_gate_up[None],
                grad_b_gate_up[:1], grad_wd[:, :ff], grad_wd[:, ff])

    tok_spec = P('ep', None)
    in_specs = (tok_spec, tok_spec, P(None, None), P(None), tok_spec, tok_spec, P('ep', None, None), P('ep', None), P('ep', None, None), P('ep', None))
    out_specs = (tok_spec, tok_spec, P(None, None), P(None), P('ep', None, None), P('ep', None), P('ep', None, None), P('ep', None))
    return jax.shard_map(local_block, mesh=mesh, in_specs=in_specs, out_specs=out_specs, check_vma=False)
```
